32 devices in a mesh: row: 4 (over y, core), col: 8 (over z, x).
Axes of the slice: x: 2, y: 2, z: 4, core: 2. Of those that a mesh axis runs over, the one named last changes fastest.
Arguments:
- fock: float32 [2, 8192, 8192], P(None, 'row', 'col'), may hold values from -1.1875 to 1.1875, as said below
- density: float32 [2, 8192, 8192], P(None, 'row', 'col'), may hold values from -1.09375 to 1.09375, as said below
- probe: float32 [2, 8192, 128], P(None, 'col'), may hold values from -6 to 6
Outputs:
- propagated: float32 [2, 8192, 128], P(None, 'col')
The draws below stay inside these ranges and needn't reach their ends.
Inputs may be any that keep to these rules, and one draw needn't show every extreme that they name: Hermitian: fock[0] is symmetric and fock[1] antisymmetric, exactly. Hermitian: density[0] is symmetric and density[1] antisymmetric, exactly.
All inputs are finite; a program needn't handle non-finite values.
Results may differ from the reference program's by a relative error of at most 0.00011.
Values sent between devices are 32-bit elements; how exact they have to be, the bound alone decides.
A program may use at most 128 MiB of HBM per device.

```python
import jax
import jax.numpy as jnp
from jax import lax

N = 8192
M = 128
ORDER = 1


def hermitian(key, spread):
    key_real, key_imag = jax.random.split(key, 2)
    real_base = jnp.clip(jax.random.normal(key_real, (N, N), jnp.float32), -6.0, 6.0)
    imag_base = jnp.clip(jax.random.normal(key_imag, (N, N), jnp.float32), -6.0, 6.0)
    factor = spread / jnp.sqrt(2.0 * N)
    real_part = (real_base + real_base.T) * factor
    imag_part = (imag_base - imag_base.T) * factor
    return jnp.stack([real_part, imag_part])


def draw_fock(key, part):
    return hermitian(jax.random.fold_in(key, 11), 2.0)


def draw_density(key, part):
    return hermitian(jax.random.fold_in(key, 23), 1.0)


def block_scale(rng, dims, cuts, smallest, high):
    factor_of, own = 1.0, jax.random.fold_in(rng, 6)
    for position, parts in cuts:
        draws = jnp.exp(jax.random.uniform(jax.random.fold_in(own, position), (parts,), jnp.float32, smallest / len(cuts), high / len(cuts)))
        factor_of = factor_of * jnp.repeat(draws, dims[position] // parts).reshape([-1 if axis == position else 1 for axis in range(len(dims))])
    return factor_of


def gaussian(key, dims, scale, reach, cuts=(), kind=jnp.bfloat16):
    entries = jax.random.normal(key, dims, jnp.float32) * scale
    if len(cuts) > 0:
        entries = block_scale(key, dims, cuts, -0.22, 0.18) * entries
    return jnp.clip(entries, min=-reach, max=reach).astype(kind)


def setup_inputs(seed: int = 0) -> dict:
    streams_of = jax.random.split(jax.random.key(seed), 4)
    fock = draw_fock(jax.random.fold_in(streams_of[3], 71), 0)
    density = draw_density(jax.random.fold_in(streams_of[3], 71), 0)
    probe = gaussian(streams_of[2], (2, N, M), 1.0, 6.0, ((1, 8),), jnp.float32)
    return {"fock": fock, "density": density, "probe": probe}


time_step = 0.5


def complex_product(matrix, vector):
    hp = lax.Precision.HIGHEST
    real_part = jnp.dot(matrix[0], vector[0], precision=hp, preferred_element_type=jnp.float32) - jnp.dot(matrix[1], vector[1], precision=hp, preferred_element_type=jnp.float32)
    imag_part = jnp.dot(matrix[0], vector[1], precision=hp, preferred_element_type=jnp.float32) + jnp.dot(matrix[1], vector[0], precision=hp, preferred_element_type=jnp.float32)
    return jnp.stack([real_part, imag_part])


def times_imag(vector, factor):
    return jnp.stack([-factor * vector[1], factor * vector[0]])


def series(fock, start, sign):
    current = start
    total = start
    for degree in range(1, ORDER + 1):
        current = times_imag(complex_product(fock, current), sign * time_step / degree)
        total = total + current
    return total


def reference(fock, density, probe):
    first = series(fock, probe, 1.0)
    second = complex_product(density, first)
    return series(fock, second, -1.0)
```

```python
import functools

import jax
import jax.numpy as jnp
from jax import lax
from jax.experimental import pallas as pl
from jax.experimental.pallas import tpu as pltpu
from jax.sharding import PartitionSpec as P

time_step = 0.5
MESH = pl.DeviceIdType.MESH
GROUPS = 4
STAGES = 3
CORES = 2
SLOTS = 4


def split(value):
    high = value.astype(jnp.bfloat16)
    return high, (value - high.astype(jnp.float32)).astype(jnp.bfloat16)


def dot(left, right):
    return jnp.dot(left, right, preferred_element_type=jnp.float32)


def each(n, body):
    def step(d, carry):
        body(d)
        return carry

    lax.fori_loop(0, n, step, 0)


def kernel(
    nr, nc, fock_hbm, density_hbm, probe_ref, out_ref,
    staged, high, low, vector, blocks, part, swapped, summed,
    load_sem, zs, zr, xs, xr, s1, r1, s2, r2, s3, r3,
):
    r = lax.axis_index("row")
    c = lax.axis_index("col")
    q = nc // nr
    ny = nr // CORES
    y = lax.div(r, CORES)
    k = lax.rem(r, CORES)
    z = lax.div(c, q)
    x = lax.rem(c, q)
    items = STAGES * GROUPS
    chunk = blocks.shape[4]
    group = blocks.shape[3]
    half = group // 2
    pieces = q * CORES
    m = probe_ref.shape[2]
    source = z == r
    goes_up = jnp.logical_and(z >= r, z + 1 < nr)
    goes_down = jnp.logical_and(z <= r, z >= 1)
    sender_offset = jnp.where(z > r, -1, 1)

    def order(i):
        return lax.rem(x + lax.div(i, CORES), q) * CORES + lax.rem(i, CORES)

    def load(matrix, n, index):
        i, side = lax.div(index, 2), lax.rem(index, 2)
        slot = lax.rem(n, SLOTS)
        return pltpu.make_async_copy(
            matrix.at[side, pl.ds(pl.multiple_of(order(i) * chunk, chunk), chunk), :],
            staged.at[slot], load_sem.at[slot],
        )

    total = 2 * pieces

    def start_load(n):
        @pl.when(n < total)
        def _():
            load(fock_hbm, n, n).start()

        @pl.when(jnp.logical_and(n >= total, n < 2 * total))
        def _():
            load(density_hbm, n, n - total).start()

    def take_load(n):
        which = lax.div(n, total)
        index = lax.rem(n, total)
        i, side = lax.div(index, 2), lax.rem(index, 2)
        slot = lax.rem(n, SLOTS)
        load(fock_hbm, n, index).wait()
        rows = min(64, chunk)

        def slab(j):
            where = pl.ds(pl.multiple_of(j * rows, rows), rows)
            target = pl.ds(pl.multiple_of(order(i) * chunk + j * rows, rows), rows)
            top, rest = split(staged[slot, where, :])
            high[which, side, target, :] = top
            low[which, side, target, :] = rest

        each(chunk // rows, slab)
        start_load(n + SLOTS)

    each(SLOTS, start_load)

    barrier = pltpu.get_barrier_semaphore()

    def greet(row, col):
        pl.semaphore_signal(barrier, inc=1, device_id=(row, col), device_id_type=MESH)

    for j in range(1, nr):
        greet(lax.rem(r + j, nr), c)
    for j in range(1, q):
        greet(r, z * q + lax.rem(x + j, q))

    @pl.when(z + 1 < nr)
    def _():
        greet(r, c + q)

    @pl.when(z >= 1)
    def _():
        greet(r, c - q)

    for side in range(2):
        turned = probe_ref[side].T
        for h in range(GROUPS):
            for g in range(CORES):
                vector[0, h, g, side * half:(side + 1) * half, :] = turned[
                    h * half:(h + 1) * half, g * chunk:(g + 1) * chunk
                ]

    neighbours = nr - 1 + q - 1 + jnp.where(z + 1 < nr, 1, 0) + jnp.where(z >= 1, 1, 0)
    pl.semaphore_wait(barrier, neighbours)

    def z_copy(t, g, up):
        return pltpu.make_async_remote_copy(
            src_ref=blocks.at[t, x, g], dst_ref=blocks.at[t, x, g],
            send_sem=zs.at[t, g, up], recv_sem=zr.at[t, g],
            device_id=(r, c + q if up else c - q), device_id_type=MESH,
        )

    def x_copy(t, g, j):
        return pltpu.make_async_remote_copy(
            src_ref=blocks.at[t, x, g], dst_ref=blocks.at[t, x, g],
            send_sem=xs.at[t, g, j], recv_sem=xr.at[t, g, j],
            device_id=(r, z * q + lax.rem(x + 1 + j, q)), device_id_type=MESH,
        )

    def forward(t, g):
        @pl.when(goes_up)
        def _():
            z_copy(t, g, 1).start()

        @pl.when(goes_down)
        def _():
            z_copy(t, g, 0).start()

        for j in range(q - 1):
            x_copy(t, g, j).start()

    def feed(t, g):
        blocks[t, x, g] = vector[lax.div(t, GROUPS), lax.rem(t, GROUPS), g]
        forward(t, g)

    def receive(t, g):
        @pl.when(jnp.logical_not(source))
        def _():
            pltpu.make_async_remote_copy(
                src_ref=blocks.at[t, x, g], dst_ref=blocks.at[t, x, g],
                send_sem=zs.at[t, g, 0], recv_sem=zr.at[t, g],
                device_id=(r, c + sender_offset * q), device_id_type=MESH,
            ).wait_recv()
            forward(t, g)

    @pl.when(source)
    def _():
        def first(h):
            for g in range(CORES):
                feed(h, g)

        each(GROUPS, first)

    def multiply(t, b, g, first):
        stage = lax.div(t, GROUPS)
        which = jnp.where(stage == 1, 1, 0)
        value = blocks[t, b, g]
        top, rest = split(value)
        turned_top = jnp.concatenate([top[half:], -top[:half]], axis=0)
        turned_rest = jnp.concatenate([rest[half:], -rest[:half]], axis=0)
        left = jnp.concatenate([top, rest], axis=0)
        turned_left = jnp.concatenate([turned_top, turned_rest], axis=0)
        rows = pl.ds(pl.multiple_of((b * CORES + g) * chunk, chunk), chunk)
        for o in range(CORES):
            cols = slice(o * chunk, (o + 1) * chunk)
            both = dot(left, high[which, 0, rows, cols]) + dot(turned_left, high[which, 1, rows, cols])
            fine = dot(top, low[which, 0, rows, cols]) + dot(turned_top, low[which, 1, rows, cols])
            value = both[:group] + (both[group:] + fine)
            if first:
                part[t, o] = value
            else:
                part[t, o] += value

    partner = r + 1 - 2 * k
    mine = k
    other = 1 - k

    def swap_copy(t):
        return pltpu.make_async_remote_copy(
            src_ref=part.at[t, other], dst_ref=swapped.at[t],
            send_sem=s1.at[t], recv_sem=r1.at[t],
            device_id=(partner, c), device_id_type=MESH,
        )

    def y_copy(t, j):
        return pltpu.make_async_remote_copy(
            src_ref=summed.at[t, y], dst_ref=summed.at[t, y],
            send_sem=s2.at[t, j], recv_sem=r2.at[t, j],
            device_id=(lax.rem(y + 1 + j, ny) * CORES + k, c), device_id_type=MESH,
        )

    def share_copy(t):
        where = (lax.div(t, GROUPS) + 1, lax.rem(t, GROUPS), mine)
        return pltpu.make_async_remote_copy(
            src_ref=vector.at[where], dst_ref=vector.at[where],
            send_sem=s3.at[t], recv_sem=r3.at[t],
            device_id=(partner, c), device_id_type=MESH,
        )

    def add_cores(t):
        swap_copy(t).wait_recv()
        summed[t, y] = part[t, mine] + swapped[t]
        for j in range(ny - 1):
            y_copy(t, j).start()

    def add_rows(t):
        stage = lax.div(t, GROUPS)
        h = lax.rem(t, GROUPS)
        for j in range(ny - 1):
            y_copy(t, j).wait_recv()
        value = summed[t, 0]
        for j in range(1, ny):
            value = value + summed[t, j]
        factor = jnp.where(stage == 0, time_step, jnp.where(stage == 2, -time_step, 0.0)).astype(jnp.float32)
        keep = jnp.where(stage == 1, 0.0, 1.0).astype(jnp.float32)
        plain = jnp.where(stage == 1, 1.0, 0.0).astype(jnp.float32)
        old = vector[stage, h, mine]
        vector[stage + 1, h, mine, :half, :] = keep * old[:half] + (plain * value[:half] - factor * value[half:])
        vector[stage + 1, h, mine, half:, :] = keep * old[half:] + (plain * value[half:] + factor * value[:half])
        share_copy(t).start()
        feed_next(t, mine)

    def take_share(t):
        share_copy(t).wait_recv()
        feed_next(t, other)

    def feed_next(t, g):
        @pl.when(jnp.logical_and(source, t + GROUPS < items))
        def _():
            feed(t + GROUPS, g)

    per_slot = pieces // GROUPS

    def slot(t):
        def ready(i):
            @pl.when(t == 0)
            def _():
                take_load(2 * i)
                take_load(2 * i + 1)

        receive(t, 0)

        @pl.when(t >= 1)
        def _():
            add_cores(t - 1)

        ready(0)
        multiply(t, x, 0, True)
        receive(t, 1)
        ready(1)
        multiply(t, x, 1, False)

        @pl.when(t >= 2)
        def _():
            add_rows(t - 2)

        for i in range(1, q):
            for g in range(CORES):
                ready(i * CORES + g)
                x_copy(t, g, q - 1 - i).wait_recv()
                multiply(t, lax.rem(x + i, q), g, False)

        swap_copy(t).start()

        @pl.when(t >= 2)
        def _():
            take_share(t - 2)

        @pl.when(t < GROUPS)
        def _():
            for i in range(per_slot):
                for side in range(2):
                    take_load(total + 2 * (t * per_slot + i) + side)

    each(items, slot)

    last = items - 1
    add_cores(last)
    add_rows(last - 1)
    take_share(last - 1)
    add_rows(last)
    take_share(last)

    for side in range(2):
        for g in range(CORES):
            whole = jnp.concatenate(
                [vector[STAGES, h, g, side * half:(side + 1) * half, :] for h in range(GROUPS)], axis=0
            )
            out_ref[side, g * chunk:(g + 1) * chunk, :] = whole.T

    def drain(t):
        for g in range(CORES):
            @pl.when(goes_up)
            def _():
                z_copy(t, g, 1).wait_send()

            @pl.when(goes_down)
            def _():
                z_copy(t, g, 0).wait_send()

            for j in range(q - 1):
                x_copy(t, g, j).wait_send()
        swap_copy(t).wait_send()
        for j in range(ny - 1):
            y_copy(t, j).wait_send()
        share_copy(t).wait_send()

    each(items, drain)


def solution(mesh):
    nr = mesh.shape["row"]
    nc = mesh.shape["col"]

    def shards(fock, density, probe):
        _, rows, cols = fock.shape
        m = probe.shape[2]
        q = nc // nr
        ny = nr // CORES
        group = 2 * m // GROUPS
        chunk = cols // CORES
        items = STAGES * GROUPS
        f32 = jnp.float32
        bf16 = jnp.bfloat16
        vmem = pltpu.VMEM
        sem = pltpu.SemaphoreType.DMA
        others = max(q - 1, 1)
        far = max(ny - 1, 1)
        return pl.pallas_call(
            functools.partial(kernel, nr, nc),
            out_shape=jax.ShapeDtypeStruct(probe.shape, f32),
            in_specs=[
                pl.BlockSpec(memory_space=pl.ANY),
                pl.BlockSpec(memory_space=pl.ANY),
                pl.BlockSpec(memory_space=pltpu.VMEM),
            ],
            out_specs=pl.BlockSpec(memory_space=pltpu.VMEM),
            scratch_shapes=[
                vmem((SLOTS, chunk, cols), f32),
                vmem((2, 2, rows, cols), bf16),
                vmem((2, 2, rows, cols), bf16),
                vmem((STAGES + 1, GROUPS, CORES, group, chunk), f32),
                vmem((items, q, CORES, group, chunk), f32),
                vmem((items, CORES, group, chunk), f32),
                vmem((items, group, chunk), f32),
                vmem((items, ny, group, chunk), f32),
                sem((SLOTS,)),
                sem((items, CORES, 2)),
                sem((items, CORES)),
                sem((items, CORES, others)),
                sem((items, CORES, others)),
                sem((items,)),
                sem((items,)),
                sem((items, far)),
                sem((items, far)),
                sem((items,)),
                sem((items,)),
            ],
            compiler_params=pltpu.CompilerParams(
                collective_id=0, has_side_effects=True, vmem_limit_bytes=63 * 1024 * 1024
            ),
            name="propagate",
        )(fock, density, probe)

    return jax.shard_map(
        shards,
        mesh=mesh,
        in_specs=(P(None, "row", "col"), P(None, "row", "col"), P(None, "col", None)),
        out_specs=P(None, "col", None),
        check_vma=False,
    )
```

```python
import functools

import jax
import jax.numpy as jnp
from jax import lax
from jax.experimental import pallas as pl
from jax.experimental.pallas import tpu as pltpu
from jax.sharding import PartitionSpec as P

time_step = 0.5
MESH = pl.DeviceIdType.MESH
GROUPS = 4
STAGES = 3
CORES = 2
SLOTS = 4


def split(value):
    high = value.astype(jnp.bfloat16)
    return high, (value - high.astype(jnp.float32)).astype(jnp.bfloat16)


def dot(left, right):
    return jnp.dot(left, right, preferred_element_type=jnp.float32)


def each(n, body):
    def step(d, carry):
        body(d)
        return carry

    lax.fori_loop(0, n, step, 0)


def kernel(
    nr, nc, fock_hbm, density_hbm, probe_ref, out_ref,
    staged, high, low, vector, blocks, part, swapped, summed,
    load_sem, zs, zr, xs, xr, s1, r1, s2, r2, s3, r3,
):
    r = lax.axis_index("row")
    c = lax.axis_index("col")
    q = nc // nr
    ny = nr // CORES
    y = lax.div(r, CORES)
    k = lax.rem(r, CORES)
    z = lax.div(c, q)
    x = lax.rem(c, q)
    items = STAGES * GROUPS
    chunk = blocks.shape[4]
    group = blocks.shape[3]
    half = group // 2
    pieces = q * CORES
    m = probe_ref.shape[2]
    cut = 1
    bits = CORES * cut
    width = chunk // cut
    source = z == r
    ends = jnp.logical_or(r == 0, r == nr - 1)
    near = jnp.logical_and(ends, jnp.logical_or(z == r + 1, z == r - 1))
    goes_up = jnp.logical_and(jnp.logical_and(z >= r, z + 1 < nr), jnp.logical_not(near))
    goes_down = jnp.logical_and(jnp.logical_and(z <= r, z >= 1), jnp.logical_not(near))
    far_step = jnp.where(r == 0, 2, -2)
    goes_far = jnp.logical_and(jnp.logical_and(ends, source), nr > 2)

    def order(i):
        b = jnp.where(i < 2, 0, 1 + lax.rem(i - 2, max(q - 1, 1)))
        g = jnp.where(i < 2, i, lax.div(i - 2, max(q - 1, 1)))
        return lax.rem(x + b, q) * CORES + g

    def load(matrix, n, index):
        i, side = lax.div(index, 2), lax.rem(index, 2)
        slot = lax.rem(n, SLOTS)
        return pltpu.make_async_copy(
            matrix.at[side, pl.ds(pl.multiple_of(order(i) * chunk, chunk), chunk), :],
            staged.at[slot], load_sem.at[slot],
        )

    total = 2 * pieces

    def start_load(n):
        @pl.when(n < total)
        def _():
            load(fock_hbm, n, n).start()

        @pl.when(jnp.logical_and(n >= total, n < 2 * total))
        def _():
            load(density_hbm, n, n - total).start()

    def take_load(n):
        which = lax.div(n, total)
        index = lax.rem(n, total)
        i, side = lax.div(index, 2), lax.rem(index, 2)
        slot = lax.rem(n, SLOTS)
        load(fock_hbm, n, index).wait()
        rows = min(64, chunk)

        def slab(j):
            where = pl.ds(pl.multiple_of(j * rows, rows), rows)
            target = pl.ds(pl.multiple_of(order(i) * chunk + j * rows, rows), rows)
            top, rest = split(staged[slot, where, :])
            high[which, side, target, :] = top
            low[which, side, target, :] = rest

        each(chunk // rows, slab)
        start_load(n + SLOTS)

    each(SLOTS, start_load)

    barrier = pltpu.get_barrier_semaphore()

    def greet(row, col):
        pl.semaphore_signal(barrier, inc=1, device_id=(row, col), device_id_type=MESH)

    for j in range(1, nr):
        greet(lax.rem(r + j, nr), c)
    for j in range(1, q):
        greet(r, z * q + lax.rem(x + j, q))

    @pl.when(z + 1 < nr)
    def _():
        greet(r, c + q)

    @pl.when(z >= 1)
    def _():
        greet(r, c - q)

    @pl.when(z + 2 < nr)
    def _():
        greet(r, c + 2 * q)

    @pl.when(z >= 2)
    def _():
        greet(r, c - 2 * q)

    for side in range(2):
        turned = probe_ref[side].T
        for h in range(GROUPS):
            for g in range(CORES):
                vector[0, h, g, side * half:(side + 1) * half, :] = turned[
                    h * half:(h + 1) * half, g * chunk:(g + 1) * chunk
                ]

    neighbours = nr - 1 + q - 1
    for step in (1, 2):
        neighbours += jnp.where(z + step < nr, 1, 0) + jnp.where(z >= step, 1, 0)
    pl.semaphore_wait(barrier, neighbours)

    def bit(t, b):
        g, w = b // cut, b % cut
        return blocks.at[t, x, g, :, pl.ds(w * width, width)]

    def z_copy(t, b, way, step):
        return pltpu.make_async_remote_copy(
            src_ref=bit(t, b), dst_ref=bit(t, b),
            send_sem=zs.at[t, b, way], recv_sem=zr.at[t, b],
            device_id=(r, c + step * q), device_id_type=MESH,
        )

    def x_copy(t, b, j):
        return pltpu.make_async_remote_copy(
            src_ref=bit(t, b), dst_ref=bit(t, b),
            send_sem=xs.at[t, b, j], recv_sem=xr.at[t, b, j],
            device_id=(r, z * q + lax.rem(x + 1 + j, q)), device_id_type=MESH,
        )

    def each_z(t, b, act):
        @pl.when(goes_far)
        def _():
            act(z_copy(t, b, 2, far_step))

        @pl.when(goes_up)
        def _():
            act(z_copy(t, b, 1, 1))

        @pl.when(goes_down)
        def _():
            act(z_copy(t, b, 0, -1))

    def forward(t, b):
        each_z(t, b, lambda copy: copy.start())
        for j in range(q - 1):
            x_copy(t, b, j).start()

    def feed(t, g):
        blocks[t, x, g] = vector[lax.div(t, GROUPS), lax.rem(t, GROUPS), g]
        if isinstance(g, int):
            for w in range(cut):
                forward(t, g * cut + w)
        else:
            for value in range(CORES):
                @pl.when(g == value)
                def _():
                    for w in range(cut):
                        forward(t, value * cut + w)

    def receive(t, b):
        @pl.when(jnp.logical_not(source))
        def _():
            z_copy(t, b, 0, jnp.where(z > r, -1, 1)).wait_recv()
            forward(t, b)

    @pl.when(source)
    def _():
        def first(h):
            for g in range(CORES):
                feed(h, g)

        each(GROUPS, first)

    partner = r + 1 - 2 * k
    mine = k
    other = 1 - k

    def multiply(t, b, g, first, between=None):
        stage = lax.div(t, GROUPS)
        which = jnp.where(stage == 1, 1, 0)
        value = blocks[t, b, g]
        top, rest = split(value)
        turned_top = jnp.concatenate([top[half:], -top[:half]], axis=0)
        turned_rest = jnp.concatenate([rest[half:], -rest[:half]], axis=0)
        left = jnp.concatenate([top, rest], axis=0)
        turned_left = jnp.concatenate([turned_top, turned_rest], axis=0)
        rows = pl.ds(pl.multiple_of((b * CORES + g) * chunk, chunk), chunk)
        for o in (other, mine):
            cols = pl.ds(pl.multiple_of(o * chunk, chunk), chunk)
            both = dot(left, high[which, 0, rows, cols]) + dot(turned_left, high[which, 1, rows, cols])
            fine = dot(top, low[which, 0, rows, cols]) + dot(turned_top, low[which, 1, rows, cols])
            value = both[:group] + (both[group:] + fine)
            if first:
                part[t, o] = value
            else:
                part[t, o] += value
            if between is not None and o is other:
                between()

    def swap_copy(t):
        return pltpu.make_async_remote_copy(
            src_ref=part.at[t, other], dst_ref=swapped.at[t],
            send_sem=s1.at[t], recv_sem=r1.at[t],
            device_id=(partner, c), device_id_type=MESH,
        )

    def y_copy(t, j):
        return pltpu.make_async_remote_copy(
            src_ref=summed.at[t, y], dst_ref=summed.at[t, y],
            send_sem=s2.at[t, j], recv_sem=r2.at[t, j],
            device_id=(lax.rem(y + 1 + j, ny) * CORES + k, c), device_id_type=MESH,
        )

    def share_copy(t):
        where = (lax.div(t, GROUPS) + 1, lax.rem(t, GROUPS), mine)
        return pltpu.make_async_remote_copy(
            src_ref=vector.at[where], dst_ref=vector.at[where],
            send_sem=s3.at[t], recv_sem=r3.at[t],
            device_id=(partner, c), device_id_type=MESH,
        )

    def add_cores(t):
        swap_copy(t).wait_recv()
        summed[t, y] = part[t, mine] + swapped[t]
        for j in range(ny - 1):
            y_copy(t, j).start()

    def add_rows(t):
        stage = lax.div(t, GROUPS)
        h = lax.rem(t, GROUPS)
        for j in range(ny - 1):
            y_copy(t, j).wait_recv()
        value = summed[t, 0]
        for j in range(1, ny):
            value = value + summed[t, j]
        factor = jnp.where(stage == 0, time_step, jnp.where(stage == 2, -time_step, 0.0)).astype(jnp.float32)
        keep = jnp.where(stage == 1, 0.0, 1.0).astype(jnp.float32)
        plain = jnp.where(stage == 1, 1.0, 0.0).astype(jnp.float32)
        old = vector[stage, h, mine]
        vector[stage + 1, h, mine, :half, :] = keep * old[:half] + (plain * value[:half] - factor * value[half:])
        vector[stage + 1, h, mine, half:, :] = keep * old[half:] + (plain * value[half:] + factor * value[:half])
        share_copy(t).start()
        feed_next(t, mine)

    def take_share(t):
        share_copy(t).wait_recv()
        feed_next(t, other)

    def feed_next(t, g):
        @pl.when(jnp.logical_and(source, t + GROUPS < items))
        def _():
            feed(t + GROUPS, g)

    points = 2 * (GROUPS - 2)
    per_point = -(-total // points)
    rest = CORES - 1

    def take_fock(i):
        take_load(2 * i)
        take_load(2 * i + 1)

    def take_density(point):
        def one(i):
            n = total + point * per_point + i

            @pl.when(n < 2 * total)
            def _():
                take_load(n)

        each(per_point, one)

    def wait_x(t, g, i):
        x_copy(t, g, q - 1 - i).wait_recv()

    def finish(t):
        for i in range(1, q):
            wait_x(t, rest, i)
            last_one = i == q - 1
            multiply(t, lax.rem(x + i, q), rest, False, (lambda: swap_copy(t).start()) if last_one else None)

    def cross(t):
        for i in range(1, q):
            wait_x(t, 0, i)
            multiply(t, lax.rem(x + i, q), 0, False)

    def slot(t):
        filling = jnp.logical_and(t >= 2, t < GROUPS)

        @pl.when(t == 1)
        def _():
            take_fock(0)

        @pl.when(t >= 1)
        def _():
            multiply(t - 1, x, 0, True)

        @pl.when(t == 1)
        def _():
            take_fock(1)

        @pl.when(t >= 1)
        def _():
            multiply(t - 1, x, 1, False)

        @pl.when(t >= 3)
        def _():
            add_rows(t - 3)

        @pl.when(t >= 2)
        def _():
            add_cores(t - 2)

        @pl.when(t == 1)
        def _():
            for i in range(1, q):
                take_fock(q - 1 + i)

        @pl.when(t >= 1)
        def _():
            cross(t - 1)

        receive(t, 0)

        @pl.when(t >= 3)
        def _():
            take_share(t - 3)

        @pl.when(filling)
        def _():
            take_density(2 * (t - 2) + 0)

        @pl.when(t == 1)
        def _():
            for i in range(1, q):
                take_fock(q + i)

        @pl.when(t >= 1)
        def _():
            finish(t - 1)

        receive(t, 1)

        @pl.when(filling)
        def _():
            take_density(2 * (t - 2) + 1)

    each(items, slot)

    last = items - 1
    multiply(last, x, 0, True)
    multiply(last, x, 1, False)
    add_rows(last - 2)
    add_cores(last - 1)
    cross(last)
    take_share(last - 2)
    finish(last)
    add_rows(last - 1)
    add_cores(last)
    take_share(last - 1)
    add_rows(last)
    take_share(last)

    for side in range(2):
        for g in range(CORES):
            whole = jnp.concatenate(
                [vector[STAGES, h, g, side * half:(side + 1) * half, :] for h in range(GROUPS)], axis=0
            )
            out_ref[side, g * chunk:(g + 1) * chunk, :] = whole.T

    def drain(t):
        for b in range(bits):
            each_z(t, b, lambda copy: copy.wait_send())
            for j in range(q - 1):
                x_copy(t, b, j).wait_send()
        swap_copy(t).wait_send()
        for j in range(ny - 1):
            y_copy(t, j).wait_send()
        share_copy(t).wait_send()

    each(items, drain)


def solution(mesh):
    nr = mesh.shape["row"]
    nc = mesh.shape["col"]

    def shards(fock, density, probe):
        _, rows, cols = fock.shape
        m = probe.shape[2]
        q = nc // nr
        ny = nr // CORES
        group = 2 * m // GROUPS
        chunk = cols // CORES
        items = STAGES * GROUPS
        bits = CORES
        f32 = jnp.float32
        bf16 = jnp.bfloat16
        vmem = pltpu.VMEM
        sem = pltpu.SemaphoreType.DMA
        others = max(q - 1, 1)
        far = max(ny - 1, 1)
        return pl.pallas_call(
            functools.partial(kernel, nr, nc),
            out_shape=jax.ShapeDtypeStruct(probe.shape, f32),
            in_specs=[
                pl.BlockSpec(memory_space=pl.ANY),
                pl.BlockSpec(memory_space=pl.ANY),
                pl.BlockSpec(memory_space=pltpu.VMEM),
            ],
            out_specs=pl.BlockSpec(memory_space=pltpu.VMEM),
            scratch_shapes=[
                vmem((SLOTS, chunk, cols), f32),
                vmem((2, 2, rows, cols), bf16),
                vmem((2, 2, rows, cols), bf16),
                vmem((STAGES + 1, GROUPS, CORES, group, chunk), f32),
                vmem((items, q, CORES, group, chunk), f32),
                vmem((items, CORES, group, chunk), f32),
                vmem((items, group, chunk), f32),
                vmem((items, ny, group, chunk), f32),
                sem((SLOTS,)),
                sem((items, bits, 3)),
                sem((items, bits)),
                sem((items, bits, others)),
                sem((items, bits, others)),
                sem((items,)),
                sem((items,)),
                sem((items, far)),
                sem((items, far)),
                sem((items,)),
                sem((items,)),
            ],
            compiler_params=pltpu.CompilerParams(
                collective_id=0, has_side_effects=True, vmem_limit_bytes=63 * 1024 * 1024
            ),
            name="propagate",
        )(fock, density, probe)

    return jax.shard_map(
        shards,
        mesh=mesh,
        in_specs=(P(None, "row", "col"), P(None, "row", "col"), P(None, "col", None)),
        out_specs=P(None, "col", None),
        check_vma=False,
    )
```

```python
import functools

import jax
import jax.numpy as jnp
from jax import lax
from jax.experimental import pallas as pl
from jax.experimental.pallas import tpu as pltpu
from jax.sharding import PartitionSpec as P

time_step = 0.5
MESH = pl.DeviceIdType.MESH
GROUPS = 4
STAGES = 3
CORES = 2
SLOTS = 4


def split(value):
    high = value.astype(jnp.bfloat16)
    return high, (value - high.astype(jnp.float32)).astype(jnp.bfloat16)


def dot(left, right):
    return jnp.dot(left, right, preferred_element_type=jnp.float32)


def each(n, body):
    def step(d, carry):
        body(d)
        return carry

    lax.fori_loop(0, n, step, 0)


def kernel(
    nr, nc, fock_hbm, density_hbm, probe_ref, out_ref,
    staged, high, low, vector, blocks, part, swapped, summed,
    load_sem, zs, zr, xs, xr, hs, s1, r1, s2, r2, s3, r3,
):
    r = lax.axis_index("row")
    c = lax.axis_index("col")
    q = nc // nr
    ny = nr // CORES
    y = lax.div(r, CORES)
    k = lax.rem(r, CORES)
    z = lax.div(c, q)
    x = lax.rem(c, q)
    items = STAGES * GROUPS
    chunk = blocks.shape[4]
    group = blocks.shape[3]
    half = group // 2
    pieces = q * CORES
    m = probe_ref.shape[2]
    source = z == r
    ends = jnp.logical_or(r == 0, r == nr - 1)
    near = jnp.logical_and(ends, jnp.logical_or(z == r + 1, z == r - 1)) if nr > 2 else r < 0
    goes_up = jnp.logical_and(jnp.logical_and(z >= r, z + 1 < nr), jnp.logical_not(near))
    goes_down = jnp.logical_and(jnp.logical_and(z <= r, z >= 1), jnp.logical_not(near))
    def twin(row):
        return lax.rem(lax.div(row, CORES) + 1, ny) * CORES + lax.rem(row, CORES)

    helped = nr > 2 and ny > 1
    at_end = jnp.logical_or(z == 0, z == nr - 1)
    assists = jnp.logical_and(at_end, r == twin(z)) if helped else r < 0
    assisted = c + jnp.where(z == 0, 2, -2) * q
    second = jnp.logical_and(ends, jnp.logical_or(z == r + 2, z == r - 2)) if helped else r < 0

    def order(i):
        b = jnp.where(i < 2, 0, 1 + lax.rem(i - 2, max(q - 1, 1)))
        g = jnp.where(i < 2, i, lax.div(i - 2, max(q - 1, 1)))
        return lax.rem(x + b, q) * CORES + g

    def load(matrix, n, index):
        i, side = lax.div(index, 2), lax.rem(index, 2)
        slot = lax.rem(n, SLOTS)
        return pltpu.make_async_copy(
            matrix.at[side, pl.ds(pl.multiple_of(order(i) * chunk, chunk), chunk), :],
            staged.at[slot], load_sem.at[slot],
        )

    total = 2 * pieces

    def start_load(n):
        @pl.when(n < total)
        def _():
            load(fock_hbm, n, n).start()

        @pl.when(jnp.logical_and(n >= total, n < 2 * total))
        def _():
            load(density_hbm, n, n - total).start()

    def take_load(n):
        which = lax.div(n, total)
        index = lax.rem(n, total)
        i, side = lax.div(index, 2), lax.rem(index, 2)
        slot = lax.rem(n, SLOTS)
        load(fock_hbm, n, index).wait()
        rows = min(64, chunk)

        def slab(j):
            where = pl.ds(pl.multiple_of(j * rows, rows), rows)
            target = pl.ds(pl.multiple_of(order(i) * chunk + j * rows, rows), rows)
            top, rest = split(staged[slot, where, :])
            high[which, side, target, :] = top
            low[which, side, target, :] = rest

        each(chunk // rows, slab)
        start_load(n + SLOTS)

    each(SLOTS, start_load)

    barrier = pltpu.get_barrier_semaphore()

    def greet(row, col):
        pl.semaphore_signal(barrier, inc=1, device_id=(row, col), device_id_type=MESH)

    for j in range(1, nr):
        greet(lax.rem(r + j, nr), c)
    for j in range(1, q):
        greet(r, z * q + lax.rem(x + j, q))

    @pl.when(z + 1 < nr)
    def _():
        greet(r, c + q)

    @pl.when(z >= 1)
    def _():
        greet(r, c - q)

    @pl.when(assists)
    def _():
        greet(z, assisted)

    @pl.when(second)
    def _():
        greet(twin(r), r * q + x)

    for side in range(2):
        turned = probe_ref[side].T
        for h in range(GROUPS):
            for g in range(CORES):
                vector[0, h, g, side * half:(side + 1) * half, :] = turned[
                    h * half:(h + 1) * half, g * chunk:(g + 1) * chunk
                ]

    neighbours = nr - 1 + q - 1
    for meets in (z + 1 < nr, z >= 1, assists, second):
        neighbours += jnp.where(meets, 1, 0)
    pl.semaphore_wait(barrier, neighbours)

    def z_copy(t, g, up, step):
        return pltpu.make_async_remote_copy(
            src_ref=blocks.at[t, x, g], dst_ref=blocks.at[t, x, g],
            send_sem=zs.at[t, g, up], recv_sem=zr.at[t, g],
            device_id=(r, c + step * q), device_id_type=MESH,
        )

    def x_copy(t, g, j):
        return pltpu.make_async_remote_copy(
            src_ref=blocks.at[t, x, g], dst_ref=blocks.at[t, x, g],
            send_sem=xs.at[t, g, j], recv_sem=xr.at[t, g, j],
            device_id=(r, z * q + lax.rem(x + 1 + j, q)), device_id_type=MESH,
        )

    def assist_copy(t, g):
        return pltpu.make_async_remote_copy(
            src_ref=vector.at[lax.div(t, GROUPS), lax.rem(t, GROUPS), g], dst_ref=blocks.at[t, x, g],
            send_sem=hs.at[t, g], recv_sem=zr.at[t, g],
            device_id=(z, assisted), device_id_type=MESH,
        )

    def each_z(t, g, act):
        @pl.when(goes_up)
        def _():
            act(z_copy(t, g, 1, 1))

        @pl.when(goes_down)
        def _():
            act(z_copy(t, g, 0, -1))

    def forward(t, g):
        each_z(t, g, lambda copy: copy.start())
        for j in range(q - 1):
            x_copy(t, g, j).start()

    def feed(t, g):
        @pl.when(source)
        def _():
            blocks[t, x, g] = vector[lax.div(t, GROUPS), lax.rem(t, GROUPS), g]
            forward(t, g)

        @pl.when(assists)
        def _():
            assist_copy(t, g).start()

    def receive(t, g):
        @pl.when(jnp.logical_not(source))
        def _():
            z_copy(t, g, 0, jnp.where(z > r, -1, 1)).wait_recv()
            forward(t, g)

    def first(h):
        for g in range(CORES):
            feed(h, g)

    each(GROUPS, first)

    partner = r + 1 - 2 * k
    mine = k
    other = 1 - k

    def multiply(t, b, g, first, between=None):
        stage = lax.div(t, GROUPS)
        which = jnp.where(stage == 1, 1, 0)
        value = blocks[t, b, g]
        top, rest = split(value)
        turned_top = jnp.concatenate([top[half:], -top[:half]], axis=0)
        turned_rest = jnp.concatenate([rest[half:], -rest[:half]], axis=0)
        left = jnp.concatenate([top, rest], axis=0)
        turned_left = jnp.concatenate([turned_top, turned_rest], axis=0)
        rows = pl.ds(pl.multiple_of((b * CORES + g) * chunk, chunk), chunk)
        for o in (other, mine):
            cols = pl.ds(pl.multiple_of(o * chunk, chunk), chunk)
            both = dot(left, high[which, 0, rows, cols]) + dot(turned_left, high[which, 1, rows, cols])
            fine = dot(top, low[which, 0, rows, cols]) + dot(turned_top, low[which, 1, rows, cols])
            value = both[:group] + (both[group:] + fine)
            if first:
                part[t, o] = value
            else:
                part[t, o] += value
            if between is not None and o is other:
                between()

    def swap_copy(t):
        return pltpu.make_async_remote_copy(
            src_ref=part.at[t, other], dst_ref=swapped.at[t],
            send_sem=s1.at[t], recv_sem=r1.at[t],
            device_id=(partner, c), device_id_type=MESH,
        )

    def y_copy(t, j):
        return pltpu.make_async_remote_copy(
            src_ref=summed.at[t, y], dst_ref=summed.at[t, y],
            send_sem=s2.at[t, j], recv_sem=r2.at[t, j],
            device_id=(lax.rem(y + 1 + j, ny) * CORES + k, c), device_id_type=MESH,
        )

    def share_copy(t):
        where = (lax.div(t, GROUPS) + 1, lax.rem(t, GROUPS), mine)
        return pltpu.make_async_remote_copy(
            src_ref=vector.at[where], dst_ref=vector.at[where],
            send_sem=s3.at[t], recv_sem=r3.at[t],
            device_id=(partner, c), device_id_type=MESH,
        )

    def add_cores(t):
        swap_copy(t).wait_recv()
        summed[t, y] = part[t, mine] + swapped[t]
        for j in range(ny - 1):
            y_copy(t, j).start()

    def add_rows(t):
        stage = lax.div(t, GROUPS)
        h = lax.rem(t, GROUPS)
        for j in range(ny - 1):
            y_copy(t, j).wait_recv()
        value = summed[t, 0]
        for j in range(1, ny):
            value = value + summed[t, j]
        factor = jnp.where(stage == 0, time_step, jnp.where(stage == 2, -time_step, 0.0)).astype(jnp.float32)
        keep = jnp.where(stage == 1, 0.0, 1.0).astype(jnp.float32)
        plain = jnp.where(stage == 1, 1.0, 0.0).astype(jnp.float32)
        old = vector[stage, h, mine]
        vector[stage + 1, h, mine, :half, :] = keep * old[:half] + (plain * value[:half] - factor * value[half:])
        vector[stage + 1, h, mine, half:, :] = keep * old[half:] + (plain * value[half:] + factor * value[:half])
        share_copy(t).start()
        feed_next(t, mine)

    def take_share(t):
        share_copy(t).wait_recv()
        feed_next(t, other)

    def feed_next(t, g):
        @pl.when(t + GROUPS < items)
        def _():
            feed(t + GROUPS, g)

    points = 2 * (GROUPS - 2)
    per_point = -(-total // points)
    rest = CORES - 1

    def take_fock(i):
        take_load(2 * i)
        take_load(2 * i + 1)

    def take_density(point):
        def one(i):
            n = total + point * per_point + i

            @pl.when(n < 2 * total)
            def _():
                take_load(n)

        each(per_point, one)

    def wait_x(t, g, i):
        x_copy(t, g, q - 1 - i).wait_recv()

    def finish(t):
        for i in range(1, q):
            wait_x(t, rest, i)
            last_one = i == q - 1
            multiply(t, lax.rem(x + i, q), rest, False, (lambda: swap_copy(t).start()) if last_one else None)

    def cross(t):
        for i in range(1, q):
            wait_x(t, 0, i)
            multiply(t, lax.rem(x + i, q), 0, False)

    def slot(t):
        filling = jnp.logical_and(t >= 2, t < GROUPS)

        @pl.when(t >= 2)
        def _():
            add_cores(t - 2)

        @pl.when(t == 1)
        def _():
            take_fock(1)

        @pl.when(t >= 1)
        def _():
            multiply(t - 1, x, 1, False)

        @pl.when(t == 1)
        def _():
            for i in range(1, q):
                take_fock(q - 1 + i)

        @pl.when(t >= 1)
        def _():
            cross(t - 1)

        @pl.when(t >= 3)
        def _():
            take_share(t - 3)

        receive(t, 0)

        @pl.when(filling)
        def _():
            take_density(2 * (t - 2) + 0)

        @pl.when(t == 0)
        def _():
            take_fock(0)

        multiply(t, x, 0, True)

        @pl.when(t == 1)
        def _():
            for i in range(1, q):
                take_fock(q + i)

        @pl.when(t >= 1)
        def _():
            finish(t - 1)

        receive(t, 1)

        @pl.when(t >= 2)
        def _():
            add_rows(t - 2)

        @pl.when(filling)
        def _():
            take_density(2 * (t - 2) + 1)

    each(items, slot)

    last = items - 1
    add_cores(last - 1)
    multiply(last, x, 1, False)
    cross(last)
    take_share(last - 2)
    finish(last)
    add_rows(last - 1)
    add_cores(last)
    take_share(last - 1)
    add_rows(last)
    take_share(last)

    for side in range(2):
        for g in range(CORES):
            whole = jnp.concatenate(
                [vector[STAGES, h, g, side * half:(side + 1) * half, :] for h in range(GROUPS)], axis=0
            )
            out_ref[side, g * chunk:(g + 1) * chunk, :] = whole.T

    def drain(t):
        for g in range(CORES):
            each_z(t, g, lambda copy: copy.wait_send())
            for j in range(q - 1):
                x_copy(t, g, j).wait_send()

            @pl.when(assists)
            def _():
                assist_copy(t, g).wait_send()
        swap_copy(t).wait_send()
        for j in range(ny - 1):
            y_copy(t, j).wait_send()
        share_copy(t).wait_send()

    each(items, drain)


def solution(mesh):
    nr = mesh.shape["row"]
    nc = mesh.shape["col"]

    def shards(fock, density, probe):
        _, rows, cols = fock.shape
        m = probe.shape[2]
        q = nc // nr
        ny = nr // CORES
        group = 2 * m // GROUPS
        chunk = cols // CORES
        items = STAGES * GROUPS
        f32 = jnp.float32
        bf16 = jnp.bfloat16
        vmem = pltpu.VMEM
        sem = pltpu.SemaphoreType.DMA
        others = max(q - 1, 1)
        far = max(ny - 1, 1)
        return pl.pallas_call(
            functools.partial(kernel, nr, nc),
            out_shape=jax.ShapeDtypeStruct(probe.shape, f32),
            in_specs=[
                pl.BlockSpec(memory_space=pl.ANY),
                pl.BlockSpec(memory_space=pl.ANY),
                pl.BlockSpec(memory_space=pltpu.VMEM),
            ],
            out_specs=pl.BlockSpec(memory_space=pltpu.VMEM),
            scratch_shapes=[
                vmem((SLOTS, chunk, cols), f32),
                vmem((2, 2, rows, cols), bf16),
                vmem((2, 2, rows, cols), bf16),
                vmem((STAGES + 1, GROUPS, CORES, group, chunk), f32),
                vmem((items, q, CORES, group, chunk), f32),
                vmem((items, CORES, group, chunk), f32),
                vmem((items, group, chunk), f32),
                vmem((items, ny, group, chunk), f32),
                sem((SLOTS,)),
                sem((items, CORES, 2)),
                sem((items, CORES)),
                sem((items, CORES, others)),
                sem((items, CORES, others)),
                sem((items, CORES)),
                sem((items,)),
                sem((items,)),
                sem((items, far)),
                sem((items, far)),
                sem((items,)),
                sem((items,)),
            ],
            compiler_params=pltpu.CompilerParams(
                collective_id=0, has_side_effects=True, vmem_limit_bytes=63 * 1024 * 1024
            ),
            name="propagate",
        )(fock, density, probe)

    return jax.shard_map(
        shards,
        mesh=mesh,
        in_specs=(P(None, "row", "col"), P(None, "row", "col"), P(None, "col", None)),
        out_specs=P(None, "col", None),
        check_vma=False,
    )
```

```python
import functools

import jax
import jax.numpy as jnp
from jax import lax
from jax.experimental import pallas as pl
from jax.experimental.pallas import tpu as pltpu
from jax.sharding import PartitionSpec as P

time_step = 0.5
MESH = pl.DeviceIdType.MESH
GROUPS = 4
STAGES = 3
CORES = 2
SLOTS = 4


def split(value):
    high = value.astype(jnp.bfloat16)
    return high, (value - high.astype(jnp.float32)).astype(jnp.bfloat16)


def dot(left, right):
    return jnp.dot(left, right, preferred_element_type=jnp.float32)


def each(n, body):
    def step(d, carry):
        body(d)
        return carry

    lax.fori_loop(0, n, step, 0)


def kernel(
    nr, nc, fock_hbm, density_hbm, probe_ref, out_ref,
    staged, high, low, vector, blocks, part, swapped, summed,
    load_sem, zs, zr, xs, xr, hs, s1, r1, s2, r2, s3, r3,
):
    r = lax.axis_index("row")
    c = lax.axis_index("col")
    q = nc // nr
    ny = nr // CORES
    y = lax.div(r, CORES)
    k = lax.rem(r, CORES)
    z = lax.div(c, q)
    x = lax.rem(c, q)
    items = STAGES * GROUPS
    chunk = blocks.shape[4]
    group = blocks.shape[3]
    half = group // 2
    pieces = q * CORES
    m = probe_ref.shape[2]
    source = z == r
    ends = jnp.logical_or(r == 0, r == nr - 1)
    inner = jnp.logical_not(ends)
    near = jnp.logical_or(z == r + 1, z == r - 1) if nr > 2 else r < 0
    goes_up = jnp.logical_and(jnp.logical_and(z >= r, z + 1 < nr), jnp.logical_not(near))
    goes_down = jnp.logical_and(jnp.logical_and(z <= r, z >= 1), jnp.logical_not(near))
    def twin(row):
        return lax.rem(lax.div(row, CORES) + 1, ny) * CORES + lax.rem(row, CORES)

    helped = nr > 2 and ny > 1
    at_end = jnp.logical_or(z == 0, z == nr - 1)
    assists = jnp.logical_and(at_end, r == twin(z)) if helped else r < 0
    assisted = c + jnp.where(z == 0, 2, -2) * q
    second = jnp.logical_and(ends, jnp.logical_or(z == r + 2, z == r - 2)) if helped else r < 0

    far_up = jnp.logical_and(jnp.logical_and(source, inner), z + 2 < nr)
    far_down = jnp.logical_and(jnp.logical_and(source, inner), z >= 2)
    from_below = jnp.logical_and(inner, z == r + 2)
    from_above = jnp.logical_and(inner, z == r - 2)

    def order(i):
        b = jnp.where(i < 2, 0, 1 + lax.rem(i - 2, max(q - 1, 1)))
        g = jnp.where(i < 2, i, lax.div(i - 2, max(q - 1, 1)))
        return lax.rem(x + b, q) * CORES + g

    def load(matrix, n, index):
        i, side = lax.div(index, 2), lax.rem(index, 2)
        slot = lax.rem(n, SLOTS)
        return pltpu.make_async_copy(
            matrix.at[side, pl.ds(pl.multiple_of(order(i) * chunk, chunk), chunk), :],
            staged.at[slot], load_sem.at[slot],
        )

    total = 2 * pieces

    def start_load(n):
        @pl.when(n < total)
        def _():
            load(fock_hbm, n, n).start()

        @pl.when(jnp.logical_and(n >= total, n < 2 * total))
        def _():
            load(density_hbm, n, n - total).start()

    def take_load(n):
        which = lax.div(n, total)
        index = lax.rem(n, total)
        i, side = lax.div(index, 2), lax.rem(index, 2)
        slot = lax.rem(n, SLOTS)
        load(fock_hbm, n, index).wait()
        rows = min(64, chunk)

        def slab(j):
            where = pl.ds(pl.multiple_of(j * rows, rows), rows)
            target = pl.ds(pl.multiple_of(order(i) * chunk + j * rows, rows), rows)
            top, rest = split(staged[slot, where, :])
            high[which, side, target, :] = top
            low[which, side, target, :] = rest

        each(chunk // rows, slab)
        start_load(n + SLOTS)

    each(SLOTS, start_load)

    barrier = pltpu.get_barrier_semaphore()

    def greet(row, col):
        pl.semaphore_signal(barrier, inc=1, device_id=(row, col), device_id_type=MESH)

    for j in range(1, nr):
        greet(lax.rem(r + j, nr), c)
    for j in range(1, q):
        greet(r, z * q + lax.rem(x + j, q))

    @pl.when(z + 1 < nr)
    def _():
        greet(r, c + q)

    @pl.when(z >= 1)
    def _():
        greet(r, c - q)

    @pl.when(assists)
    def _():
        greet(z, assisted)

    @pl.when(second)
    def _():
        greet(twin(r), r * q + x)

    @pl.when(jnp.logical_or(far_up, from_above))
    def _():
        greet(r, c + 2 * q)

    @pl.when(jnp.logical_or(far_down, from_below))
    def _():
        greet(r, c - 2 * q)

    for side in range(2):
        turned = probe_ref[side].T
        for h in range(GROUPS):
            for g in range(CORES):
                vector[0, h, g, side * half:(side + 1) * half, :] = turned[
                    h * half:(h + 1) * half, g * chunk:(g + 1) * chunk
                ]

    neighbours = nr - 1 + q - 1
    for meets in (z + 1 < nr, z >= 1, assists, second, far_up, far_down, from_below, from_above):
        neighbours += jnp.where(meets, 1, 0)
    pl.semaphore_wait(barrier, neighbours)

    def z_copy(t, g, up, step):
        return pltpu.make_async_remote_copy(
            src_ref=blocks.at[t, x, g], dst_ref=blocks.at[t, x, g],
            send_sem=zs.at[t, g, up], recv_sem=zr.at[t, g],
            device_id=(r, c + step * q), device_id_type=MESH,
        )

    def x_copy(t, g, j):
        return pltpu.make_async_remote_copy(
            src_ref=blocks.at[t, x, g], dst_ref=blocks.at[t, x, g],
            send_sem=xs.at[t, g, j], recv_sem=xr.at[t, g, j],
            device_id=(r, z * q + lax.rem(x + 1 + j, q)), device_id_type=MESH,
        )

    def assist_copy(t, g):
        return pltpu.make_async_remote_copy(
            src_ref=vector.at[lax.div(t, GROUPS), lax.rem(t, GROUPS), g], dst_ref=blocks.at[t, x, g],
            send_sem=hs.at[t, g], recv_sem=zr.at[t, g],
            device_id=(z, assisted), device_id_type=MESH,
        )

    def each_z(t, g, act):
        @pl.when(far_up)
        def _():
            act(z_copy(t, g, 3, 2))

        @pl.when(far_down)
        def _():
            act(z_copy(t, g, 2, -2))

        @pl.when(goes_up)
        def _():
            act(z_copy(t, g, 1, 1))

        @pl.when(goes_down)
        def _():
            act(z_copy(t, g, 0, -1))

    def forward(t, g):
        each_z(t, g, lambda copy: copy.start())
        for j in range(q - 1):
            x_copy(t, g, j).start()

    def feed(t, g):
        @pl.when(source)
        def _():
            blocks[t, x, g] = vector[lax.div(t, GROUPS), lax.rem(t, GROUPS), g]
            forward(t, g)

        @pl.when(assists)
        def _():
            assist_copy(t, g).start()

    def receive(t, g):
        @pl.when(jnp.logical_not(source))
        def _():
            z_copy(t, g, 0, jnp.where(z > r, -1, 1)).wait_recv()
            forward(t, g)

    def first(h):
        for g in range(CORES):
            feed(h, g)

    each(GROUPS, first)

    partner = r + 1 - 2 * k
    mine = k
    other = 1 - k

    def multiply(t, b, g, first, between=None):
        stage = lax.div(t, GROUPS)
        which = jnp.where(stage == 1, 1, 0)
        value = blocks[t, b, g]
        top, rest = split(value)
        turned_top = jnp.concatenate([top[half:], -top[:half]], axis=0)
        turned_rest = jnp.concatenate([rest[half:], -rest[:half]], axis=0)
        left = jnp.concatenate([top, rest], axis=0)
        turned_left = jnp.concatenate([turned_top, turned_rest], axis=0)
        rows = pl.ds(pl.multiple_of((b * CORES + g) * chunk, chunk), chunk)
        for o in (other, mine):
            cols = pl.ds(pl.multiple_of(o * chunk, chunk), chunk)
            both = dot(left, high[which, 0, rows, cols]) + dot(turned_left, high[which, 1, rows, cols])
            fine = dot(top, low[which, 0, rows, cols]) + dot(turned_top, low[which, 1, rows, cols])
            value = both[:group] + (both[group:] + fine)
            if first:
                part[t, o] = value
            else:
                part[t, o] += value
            if between is not None and o is other:
                between()

    def swap_copy(t):
        return pltpu.make_async_remote_copy(
            src_ref=part.at[t, other], dst_ref=swapped.at[t],
            send_sem=s1.at[t], recv_sem=r1.at[t],
            device_id=(partner, c), device_id_type=MESH,
        )

    def y_copy(t, j):
        return pltpu.make_async_remote_copy(
            src_ref=summed.at[t, y], dst_ref=summed.at[t, y],
            send_sem=s2.at[t, j], recv_sem=r2.at[t, j],
            device_id=(lax.rem(y + 1 + j, ny) * CORES + k, c), device_id_type=MESH,
        )

    def share_copy(t):
        where = (lax.div(t, GROUPS) + 1, lax.rem(t, GROUPS), mine)
        return pltpu.make_async_remote_copy(
            src_ref=vector.at[where], dst_ref=vector.at[where],
            send_sem=s3.at[t], recv_sem=r3.at[t],
            device_id=(partner, c), device_id_type=MESH,
        )

    def add_cores(t):
        swap_copy(t).wait_recv()
        summed[t, y] = part[t, mine] + swapped[t]
        for j in range(ny - 1):
            y_copy(t, j).start()

    def add_rows(t):
        stage = lax.div(t, GROUPS)
        h = lax.rem(t, GROUPS)
        for j in range(ny - 1):
            y_copy(t, j).wait_recv()
        value = summed[t, 0]
        for j in range(1, ny):
            value = value + summed[t, j]
        factor = jnp.where(stage == 0, time_step, jnp.where(stage == 2, -time_step, 0.0)).astype(jnp.float32)
        keep = jnp.where(stage == 1, 0.0, 1.0).astype(jnp.float32)
        plain = jnp.where(stage == 1, 1.0, 0.0).astype(jnp.float32)
        old = vector[stage, h, mine]
        vector[stage + 1, h, mine, :half, :] = keep * old[:half] + (plain * value[:half] - factor * value[half:])
        vector[stage + 1, h, mine, half:, :] = keep * old[half:] + (plain * value[half:] + factor * value[:half])
        share_copy(t).start()
        feed_next(t, mine)

    def take_share(t):
        share_copy(t).wait_recv()
        feed_next(t, other)

    def feed_next(t, g):
        @pl.when(t + GROUPS < items)
        def _():
            feed(t + GROUPS, g)

    points = 2 * (GROUPS - 2)
    per_point = -(-total // points)
    rest = CORES - 1

    def take_fock(i):
        take_load(2 * i)
        take_load(2 * i + 1)

    def take_density(point):
        def one(i):
            n = total + point * per_point + i

            @pl.when(n < 2 * total)
            def _():
                take_load(n)

        each(per_point, one)

    def wait_x(t, g, i):
        x_copy(t, g, q - 1 - i).wait_recv()

    def finish(t):
        for i in range(1, q):
            wait_x(t, rest, i)
            last_one = i == q - 1
            multiply(t, lax.rem(x + i, q), rest, False, (lambda: swap_copy(t).start()) if last_one else None)

    def cross(t):
        for i in range(1, q):
            wait_x(t, 0, i)
            multiply(t, lax.rem(x + i, q), 0, False)

    def slot(t):
        filling = jnp.logical_and(t >= 2, t < GROUPS)

        @pl.when(t >= 2)
        def _():
            add_cores(t - 2)

        @pl.when(t == 1)
        def _():
            take_fock(1)

        @pl.when(t >= 1)
        def _():
            multiply(t - 1, x, 1, False)

        @pl.when(t == 1)
        def _():
            for i in range(1, q):
                take_fock(q - 1 + i)

        @pl.when(t >= 1)
        def _():
            cross(t - 1)

        @pl.when(t >= 3)
        def _():
            take_share(t - 3)

        receive(t, 0)

        @pl.when(filling)
        def _():
            take_density(2 * (t - 2) + 0)

        @pl.when(t == 0)
        def _():
            take_fock(0)

        multiply(t, x, 0, True)

        @pl.when(t == 1)
        def _():
            for i in range(1, q):
                take_fock(q + i)

        @pl.when(t >= 1)
        def _():
            finish(t - 1)

        receive(t, 1)

        @pl.when(t >= 2)
        def _():
            add_rows(t - 2)

        @pl.when(filling)
        def _():
            take_density(2 * (t - 2) + 1)

    each(items, slot)

    last = items - 1
    add_cores(last - 1)
    multiply(last, x, 1, False)
    cross(last)
    take_share(last - 2)
    finish(last)
    add_rows(last - 1)
    add_cores(last)
    take_share(last - 1)
    add_rows(last)
    take_share(last)

    for side in range(2):
        for g in range(CORES):
            whole = jnp.concatenate(
                [vector[STAGES, h, g, side * half:(side + 1) * half, :] for h in range(GROUPS)], axis=0
            )
            out_ref[side, g * chunk:(g + 1) * chunk, :] = whole.T

    def drain(t):
        for g in range(CORES):
            each_z(t, g, lambda copy: copy.wait_send())
            for j in range(q - 1):
                x_copy(t, g, j).wait_send()

            @pl.when(assists)
            def _():
                assist_copy(t, g).wait_send()
        swap_copy(t).wait_send()
        for j in range(ny - 1):
            y_copy(t, j).wait_send()
        share_copy(t).wait_send()

    each(items, drain)


def solution(mesh):
    nr = mesh.shape["row"]
    nc = mesh.shape["col"]

    def shards(fock, density, probe):
        _, rows, cols = fock.shape
        m = probe.shape[2]
        q = nc // nr
        ny = nr // CORES
        group = 2 * m // GROUPS
        chunk = cols // CORES
        items = STAGES * GROUPS
        f32 = jnp.float32
        bf16 = jnp.bfloat16
        vmem = pltpu.VMEM
        sem = pltpu.SemaphoreType.DMA
        others = max(q - 1, 1)
        far = max(ny - 1, 1)
        return pl.pallas_call(
            functools.partial(kernel, nr, nc),
            out_shape=jax.ShapeDtypeStruct(probe.shape, f32),
            in_specs=[
                pl.BlockSpec(memory_space=pl.ANY),
                pl.BlockSpec(memory_space=pl.ANY),
                pl.BlockSpec(memory_space=pltpu.VMEM),
            ],
            out_specs=pl.BlockSpec(memory_space=pltpu.VMEM),
            scratch_shapes=[
                vmem((SLOTS, chunk, cols), f32),
                vmem((2, 2, rows, cols), bf16),
                vmem((2, 2, rows, cols), bf16),
                vmem((STAGES + 1, GROUPS, CORES, group, chunk), f32),
                vmem((items, q, CORES, group, chunk), f32),
                vmem((items, CORES, group, chunk), f32),
                vmem((items, group, chunk), f32),
                vmem((items, ny, group, chunk), f32),
                sem((SLOTS,)),
                sem((items, CORES, 4)),
                sem((items, CORES)),
                sem((items, CORES, others)),
                sem((items, CORES, others)),
                sem((items, CORES)),
                sem((items,)),
                sem((items,)),
                sem((items, far)),
                sem((items, far)),
                sem((items,)),
                sem((items,)),
            ],
            compiler_params=pltpu.CompilerParams(
                collective_id=0, has_side_effects=True, vmem_limit_bytes=63 * 1024 * 1024
            ),
            name="propagate",
        )(fock, density, probe)

    return jax.shard_map(
        shards,
        mesh=mesh,
        in_specs=(P(None, "row", "col"), P(None, "row", "col"), P(None, "col", None)),
        out_specs=P(None, "col", None),
        check_vma=False,
    )
```
